32 devices in a mesh: dp: 2 (over x), ctx: 4 (over y, core), tp: 4 (over z).
Axes of the slice: x: 2, y: 2, z: 4, core: 2. Of those that a mesh axis runs over, the one named last changes fastest.
Arguments:
- layer_input: bfloat16 [2, 1024, 8192], P('dp', ('ctx', 'tp')), may hold values from -6 to 6
- value_weight: bfloat16 [8192, 1024], P(('dp', 'ctx'), 'tp'), may hold values from -0.0625 to 0.0625
- query_raw: bfloat16 [2, 1024, 1024], P('dp', 'ctx', 'tp'), may hold values from -6 to 6
- key_raw: bfloat16 [2, 1024, 1024], P('dp', 'ctx', 'tp'), may hold values from -6 to 6
- out_grad: bfloat16 [2, 1024, 1024], P('dp', 'ctx', 'tp'), may hold values from -6 to 6
- gate_logits: float32 [2, 2, 8, 1024], P(None, 'dp', 'tp', 'ctx'), may hold values from -14 to 4, as said below
- decay_params: float32 [2, 8], P(None, 'tp'), may hold values from -0.35 to 0.35
- saved_states: float32 [2, 4, 8, 128, 128], P('dp', 'ctx', 'tp'), may hold values from -4 to 4
Outputs:
- input_grad: bfloat16 [2, 1024, 8192], P('dp', ('ctx', 'tp'))
- query_grad: bfloat16 [2, 1024, 1024], P('dp', 'ctx', 'tp')
- key_grad: bfloat16 [2, 1024, 1024], P('dp', 'ctx', 'tp')
- gate_grad: float32 [2, 2, 8, 1024], P(None, 'dp', 'tp', 'ctx')
- decay_grad: float32 [2, 8], P(None, 'tp')
The draws below stay inside these ranges and needn't reach their ends.
Inputs may be any that keep to these rules, and one draw needn't show every extreme that they name: `gate_logits`: row 0 holds decay logits, row 1 write-strength logits.
All inputs are finite; a program needn't handle non-finite values.
Results may differ from the reference program's by a relative error of at most 0.015.
Values may be sent and summed in bfloat16 or wider, within the bound.
No kernel may reach another device: no remote copies, remote signals or barrier semaphores. Data moves between devices by JAX's collectives and lax.ppermute only.
A program may use at most 64 MiB of HBM per device.

```python
import math
import jax
import jax.numpy as jnp
from jax import lax

D = 8192
HD = 128
HEADS_DEV = 2
SUBLEN = 64
TOK_DEV = 256
LOCAL_HEADS = 8
BATCH_SEQUENCES = 2
BLOCKS = 4
SEQUENCE_TOKENS = 1024


def draw_gate_logits(key, part):
    random_subkeys = jax.random.split(key, 8)
    fast_share = 0.5
    shape_head = (BATCH_SEQUENCES, LOCAL_HEADS, 1)
    is_fast = jax.random.uniform(random_subkeys[0], shape_head) < fast_share
    fast_rate = jnp.exp(jax.random.uniform(random_subkeys[1], shape_head, minval=math.log(0.02), maxval=math.log(0.05)))
    slow_rate = jnp.exp(jax.random.uniform(random_subkeys[2], shape_head, minval=math.log(0.1), maxval=math.log(0.5))) / SEQUENCE_TOKENS
    baseline_rate = jnp.where(is_fast, fast_rate, slow_rate)
    block_scaling = jnp.exp(jax.random.uniform(random_subkeys[3], (BATCH_SEQUENCES, LOCAL_HEADS, SEQUENCE_TOKENS // TOK_DEV, 1), minval=math.log(0.5), maxval=math.log(2.0)))
    block_scaling = jnp.broadcast_to(block_scaling, (BATCH_SEQUENCES, LOCAL_HEADS, SEQUENCE_TOKENS // TOK_DEV, TOK_DEV)).reshape(BATCH_SEQUENCES, LOCAL_HEADS, SEQUENCE_TOKENS)
    jaggedness = jnp.exp(jax.random.uniform(random_subkeys[4], (BATCH_SEQUENCES, LOCAL_HEADS, SEQUENCE_TOKENS), minval=math.log(0.5), maxval=math.log(2.0)))
    spike_events = jax.random.uniform(random_subkeys[5], (BATCH_SEQUENCES, LOCAL_HEADS, SEQUENCE_TOKENS)) < 3.0 / SEQUENCE_TOKENS
    spike_rate = jax.random.uniform(random_subkeys[6], (BATCH_SEQUENCES, LOCAL_HEADS, SEQUENCE_TOKENS), minval=0.25, maxval=0.7)
    per_token_rate = baseline_rate * block_scaling * jaggedness + jnp.where(spike_events, spike_rate, 0.0)
    decay_logit = jnp.clip(jnp.log(jnp.expm1(per_token_rate)), -14.0, 1.0)
    strength_logit = jnp.clip(1.5 * jax.random.normal(random_subkeys[7], (BATCH_SEQUENCES, LOCAL_HEADS, SEQUENCE_TOKENS)), -4.0, 4.0)
    return jnp.stack([decay_logit, strength_logit]).astype(jnp.float32)


def block_scale(rng, extent, cuts, least, largest):
    def one(axis_at, shards_of):
        draws = jax.random.uniform(jax.random.fold_in(jax.random.fold_in(rng, 6), axis_at), (shards_of,), jnp.float32, least / len(cuts), largest / len(cuts))
        return jnp.repeat(jnp.exp(draws), extent[axis_at] // shards_of).reshape((-1,) + (1,) * (len(extent) - axis_at - 1))

    loudness = one(*cuts[0])
    for cut in cuts[1:]:
        loudness = loudness * one(*cut)
    return loudness


def centred(own_key, extent, deviation, bound, cuts=(), kind=jnp.bfloat16):
    result = deviation * jax.random.normal(own_key, extent, jnp.float32)
    if cuts:
        result = result * block_scale(own_key, extent, cuts, -0.22, 0.18)
    return jnp.clip(result, -bound, bound).astype(kind)


def setup_inputs(seed: int = 0) -> dict:
    key_of = jax.random.split(jax.random.key(seed), 9)
    layer_input = centred(key_of[0], (BATCH_SEQUENCES, SEQUENCE_TOKENS, D), 1.0, 6.0, ((0, 2), (1, 16)))
    value_weight = centred(key_of[1], (D, LOCAL_HEADS * HD), D ** -0.5, 0.0625, ((0, 8), (1, 4)))
    query_raw = centred(key_of[2], (BATCH_SEQUENCES, SEQUENCE_TOKENS, LOCAL_HEADS * HD), 1.0, 6.0, ((0, 2), (1, 4), (2, 4)))
    key_raw = centred(key_of[3], (BATCH_SEQUENCES, SEQUENCE_TOKENS, LOCAL_HEADS * HD), 1.0, 6.0, ((0, 2), (1, 4), (2, 4)))
    out_grad = centred(key_of[4], (BATCH_SEQUENCES, SEQUENCE_TOKENS, LOCAL_HEADS * HD), 1.0, 6.0, ((0, 2), (1, 4), (2, 4)))
    gate_logits = draw_gate_logits(jax.random.fold_in(key_of[8], 71), 0)
    decay_params = jnp.clip(jax.random.uniform(key_of[6], (2, LOCAL_HEADS), jnp.float32, -0.35, 0.35) * block_scale(key_of[6], (2, LOCAL_HEADS), ((1, 4),), -0.4, 0.0), -0.35, 0.35)
    saved_states = centred(key_of[7], (BATCH_SEQUENCES, BLOCKS, LOCAL_HEADS, HD, HD), 0.5, 4.0, ((0, 2), (1, 4), (2, 4)), jnp.float32)
    return dict(layer_input=layer_input, value_weight=value_weight, query_raw=query_raw, key_raw=key_raw, out_grad=out_grad, gate_logits=gate_logits, decay_params=decay_params, saved_states=saved_states)


epsilon = 1e-06
highest = lax.Precision.HIGHEST

def inner_step(carried, pieces):
    query_unit, key_unit, values, log_decay, strengths = pieces
    sub_len = query_unit.shape[0]
    head_dim = query_unit.shape[1]
    cumulative = jnp.cumsum(log_decay)
    positions = jnp.arange(sub_len)
    lower_mask = positions[:, None] >= positions[None, :]
    strict_mask = positions[:, None] > positions[None, :]
    spread = jnp.where(lower_mask, cumulative[:, None] - cumulative[None, :], 0.0)
    decays = jnp.where(lower_mask, jnp.exp(spread), 0.0)
    key_gram = jnp.dot(key_unit, key_unit.T, precision=highest)
    system = jnp.eye(sub_len, dtype=jnp.float32) + jnp.where(strict_mask, strengths[:, None] * decays * key_gram, 0.0)
    right_side = jnp.concatenate([(strengths * jnp.exp(cumulative))[:, None] * key_unit, strengths[:, None] * values], axis=1)
    solved = jax.scipy.linalg.solve_triangular(system, right_side, lower=True, unit_diagonal=True)
    new_values = solved[:, head_dim:] - jnp.dot(solved[:, :head_dim], carried, precision=highest)
    scores = decays * jnp.dot(query_unit, key_unit.T, precision=highest)
    output = jnp.dot(query_unit * jnp.exp(cumulative)[:, None], carried, precision=highest) + jnp.dot(scores, new_values, precision=highest)
    tail_decay = jnp.exp(cumulative[-1] - cumulative)
    updated = jnp.exp(cumulative[-1]) * carried + jnp.dot((key_unit * tail_decay[:, None]).T, new_values, precision=highest)
    return (updated, output)

def core(query_row, key_row, values, gate_a, gate_b, params, initial):
    length = query_row.shape[0]
    head_dim = query_row.shape[1]
    query_unit = query_row * lax.rsqrt(lax.optimization_barrier(jnp.sum(query_row * query_row, axis=-1, keepdims=True)) + epsilon) * head_dim ** (-0.5)
    key_unit = key_row * lax.rsqrt(lax.optimization_barrier(jnp.sum(key_row * key_row, axis=-1, keepdims=True)) + epsilon)
    log_decay = -jnp.exp(params[0]) * jax.nn.softplus(gate_a + params[1])
    strengths = jax.nn.sigmoid(gate_b)
    blocks = length // SUBLEN

    def into_blocks(array):
        return array.reshape((blocks, SUBLEN) + array.shape[1:])
    final_state, outputs = lax.scan(inner_step, initial, (into_blocks(query_unit), into_blocks(key_unit), into_blocks(values), into_blocks(log_decay), into_blocks(strengths)))
    return (outputs.reshape(length, head_dim), final_state)

def reference(layer_input, value_weight, query_raw, key_raw, out_grad, gate_logits, decay_params, saved_states):
    batch_core = jax.vmap(core, in_axes=(0, 0, 0, 0, 0, None, 0))

    def one_head(head_index):
        columns = lax.dynamic_slice_in_dim(value_weight, head_index * HD, HD, 1)
        value_round = jnp.dot(layer_input.astype(jnp.float32), columns.astype(jnp.float32), preferred_element_type=jnp.float32).astype(jnp.bfloat16)
        value_head = value_round.astype(jnp.float32)
        query_head = lax.dynamic_slice_in_dim(query_raw, head_index * HD, HD, 2).astype(jnp.float32)
        key_head = lax.dynamic_slice_in_dim(key_raw, head_index * HD, HD, 2).astype(jnp.float32)
        grad_head = lax.dynamic_slice_in_dim(out_grad, head_index * HD, HD, 2).astype(jnp.float32)
        gates = lax.dynamic_index_in_dim(gate_logits, head_index, 2, keepdims=False)
        params = lax.dynamic_index_in_dim(decay_params, head_index, 1, keepdims=False)
        states = lax.dynamic_index_in_dim(saved_states, head_index, 2, keepdims=False)
        incoming = jnp.zeros((BATCH_SEQUENCES, HD, HD), jnp.float32)
        param_grad = jnp.zeros((2,), jnp.float32)
        collected = []
        for block_index in reversed(range(BLOCKS)):
            begin = block_index * TOK_DEV
            finish = begin + TOK_DEV
            outputs, pullback = jax.vjp(batch_core, query_head[:, begin:finish], key_head[:, begin:finish], value_head[:, begin:finish], gates[0][:, begin:finish], gates[1][:, begin:finish], params, states[:, block_index])
            gradients = pullback((grad_head[:, begin:finish], incoming))
            incoming = gradients[6]
            param_grad = param_grad + gradients[5]
            collected.append(gradients)
        collected = collected[::-1]
        query_part = jnp.concatenate([part_grads[0] for part_grads in collected], axis=1).astype(jnp.bfloat16)
        key_part = jnp.concatenate([part_grads[1] for part_grads in collected], axis=1).astype(jnp.bfloat16)
        value_part = jnp.concatenate([part_grads[2] for part_grads in collected], axis=1).astype(jnp.bfloat16)
        decay_part = jnp.concatenate([part_grads[3] for part_grads in collected], axis=1)
        strength_part = jnp.concatenate([part_grads[4] for part_grads in collected], axis=1)
        gate_part = jnp.stack([decay_part, strength_part])
        contribution = jnp.einsum('bsc,dc->bsd', value_part.astype(jnp.float32), columns.astype(jnp.float32), precision=highest)
        return (contribution, (query_part, key_part, gate_part, param_grad))

    def one_group(summed_grad, group_index):
        group_sum = jnp.zeros((BATCH_SEQUENCES, SEQUENCE_TOKENS, D), jnp.float32)
        parts = []
        for offset in range(HEADS_DEV):
            contribution, head_parts = one_head(group_index * HEADS_DEV + offset)
            group_sum = group_sum + contribution
            parts.append(head_parts)
        rounded = lax.optimization_barrier(group_sum.astype(jnp.bfloat16))
        summed_grad = summed_grad + rounded.astype(jnp.float32)
        stacked = tuple((jnp.stack([head_parts[index] for head_parts in parts]) for index in range(4)))
        return (summed_grad, stacked)
    summed, per_group = lax.scan(one_group, jnp.zeros((BATCH_SEQUENCES, SEQUENCE_TOKENS, D), jnp.float32), jnp.arange(LOCAL_HEADS // HEADS_DEV, dtype=jnp.int32))
    per_head = tuple((array.reshape((LOCAL_HEADS,) + array.shape[2:]) for array in per_group))
    query_grad = per_head[0].transpose(1, 2, 0, 3).reshape(BATCH_SEQUENCES, SEQUENCE_TOKENS, LOCAL_HEADS * HD)
    key_grad = per_head[1].transpose(1, 2, 0, 3).reshape(BATCH_SEQUENCES, SEQUENCE_TOKENS, LOCAL_HEADS * HD)
    gate_grad = per_head[2].transpose(1, 2, 0, 3)
    decay_grad = per_head[3].T
    return (summed.astype(jnp.bfloat16), query_grad, key_grad, gate_grad, decay_grad)
```

```python
import functools
import jax
import jax.numpy as jnp
from jax import lax
from jax.experimental import pallas as pl
from jax.experimental.pallas import tpu as pltpu
from jax.sharding import PartitionSpec as P

f32 = jnp.float32
bf16 = jnp.bfloat16
epsilon = 1e-06
BASE = 16


def mm(a, b, ca=1, cb=0):
    return lax.dot_general(
        a.astype(bf16), b.astype(bf16), (((ca,), (cb,)), ((), ())), preferred_element_type=f32
    )


def halves(a):
    high = a.astype(bf16)
    return high, (a - high.astype(f32)).astype(bf16)


def mm3(a, b, ca=1, cb=0):
    ah, al = halves(a)
    bh, bl = halves(b)
    return mm(ah, bh, ca, cb) + (mm(ah, bl, ca, cb) + mm(al, bh, ca, cb))


def softplus(x):
    return jnp.maximum(x, 0.0) + jnp.log(1.0 + jnp.exp(-jnp.abs(x)))


def sigmoid(x):
    return 1.0 / (1.0 + jnp.exp(-x))


def positions(n):
    return (
        lax.broadcasted_iota(jnp.int32, (n, n), 0),
        lax.broadcasted_iota(jnp.int32, (n, n), 1),
    )


def stack_rows(rows):
    n = rows[0].shape[1]
    short = -len(rows) % 8
    return jnp.concatenate(list(rows) + [jnp.zeros((1, n), f32)] * short, axis=0)


def to_columns(rows):
    turned = stack_rows(rows).T
    return [turned[:, i : i + 1] for i in range(len(rows))]


def to_rows(columns):
    n = columns[0].shape[0]
    short = -len(columns) % 8
    turned = jnp.concatenate(list(columns) + [jnp.zeros((n, 1), f32)] * short, axis=1).T
    return [turned[i : i + 1] for i in range(len(columns))]


def gate_rows(gates_ref, params_ref, heads):
    out = []
    for h in range(heads):
        ga = gates_ref[0, h : h + 1, :]
        gb = gates_ref[1, h : h + 1, :]
        scale = jnp.exp(jnp.full(ga.shape, params_ref[0, h], f32))
        shifted = ga + params_ref[1, h]
        out.append((-scale * softplus(shifted), sigmoid(gb), -scale * sigmoid(shifted)))
    return out


def cumulated(logs, i, j):
    return [jnp.sum(jnp.where(j <= i, row, 0.0), axis=1, keepdims=True) for row in logs]


def units(ref, h, hd):
    raw = ref[:, h * hd : (h + 1) * hd].astype(f32)
    inv = lax.rsqrt(jnp.sum(raw * raw, axis=-1, keepdims=True) + epsilon)
    return raw, inv


def inverse_upper(strict, i, j, dot):
    n = strict[0].shape[0]
    eye = (i == j).astype(f32)
    near = (i // BASE) == (j // BASE)
    power = [jnp.where(near, a, 0.0) for a in strict]
    result = [eye - a for a in power]
    k = 2
    while k < BASE:
        power = [dot(a, a) for a in power]
        result = [u + dot(u, a) for u, a in zip(result, power)]
        k *= 2
    b = BASE
    while b < n:
        cross = ((i // (2 * b)) == (j // (2 * b))) & ((i // b) != (j // b))
        part = [dot(u, jnp.where(cross, a, 0.0)) for u, a in zip(result, strict)]
        result = [u - dot(x, u) for u, x in zip(result, part)]
        b *= 2
    return result


def shared(gates_ref, params_ref, heads, i, j):
    rows = gate_rows(gates_ref, params_ref, heads)
    sums = cumulated([r[0] for r in rows], i, j)
    sum_rows = to_rows(sums)
    strength_cols = to_columns([r[1] for r in rows])
    return rows, sums, sum_rows, strength_cols


def kernel_a(gates_ref, params_ref, q_ref, k_ref, g_ref, bc_ref, far_ref, x_ref, z_ref, u_ref):
    heads, hd = bc_ref.shape[0], bc_ref.shape[1]
    n = q_ref.shape[0]
    i, j = positions(n)
    rows, sums, sum_rows, strengths = shared(gates_ref, params_ref, heads, i, j)
    strict, scores, ks, qs = [], [], [], []
    for h in range(heads):
        qraw, qinv = units(q_ref, h, hd)
        kraw, kinv = units(k_ref, h, hd)
        q = qraw * qinv * hd ** (-0.5)
        k = kraw * kinv
        fade = jnp.where(i <= j, jnp.exp(jnp.where(i <= j, sum_rows[h] - sums[h], 0.0)), 0.0)
        strict.append(jnp.where(i < j, fade * rows[h][1] * mm3(k, k, 1, 1), 0.0))
        scores.append(fade * mm(k, q, 1, 1))
        ks.append(k)
        qs.append(q)
    inverse = inverse_upper(strict, i, j, mm3)
    ei, ej = positions(hd)
    for h in range(heads):
        last = sums[h][n - 1 : n, :]
        tail = jnp.exp(last - sums[h])
        grown = jnp.exp(sums[h])
        cot = g_ref[:, h * hd : (h + 1) * hd]
        right = jnp.concatenate([ks[h] * tail, mm(scores[h], cot)], axis=1)
        x = mm3(inverse[h], right)
        y = mm(strengths[h] * grown * ks[h], x, 0, 0)
        b = jnp.where(ei == ej, jnp.exp(last), 0.0) - y[:, :hd]
        c = mm(qs[h] * grown, cot, 0, 0) - y[:, hd:]
        bc_ref[h] = jnp.concatenate([b, c], axis=1).astype(bf16)
        far_ref[h] = c.astype(bf16)
        x_ref[h] = x[:, :hd].astype(bf16)
        z_ref[h] = x[:, hd:]
        u_ref[h] = inverse[h]


def kernel_b(place_ref, gates_ref, x_ref, z0_ref, *refs, count, steps):
    received = refs[:count]
    outs = refs[count : count + steps]
    z_ref, end_ref, dv_ref = refs[count + steps :]
    heads, n, hd = x_ref.shape
    me = place_ref[0]
    strengths = to_columns([sigmoid(gates_ref[1, h : h + 1, :]) for h in range(heads)])
    for h in range(heads):
        end = jnp.zeros((hd, hd), f32)
        for index, ref in reversed(list(enumerate(received))):
            if index == count - 1:
                end = ref[h].astype(f32)
            else:
                end = mm(ref[h, :, :hd], end) + ref[h, :, hd:].astype(f32)
        z = z0_ref[h] + mm(x_ref[h], end)
        z_ref[h] = z
        end_ref[h] = end
        dv_ref[:, h * hd : (h + 1) * hd] = strengths[h] * z
    block = n // steps
    for m in range(steps):
        at = pl.multiple_of((me ^ m) * block, block)
        outs[m][...] = dv_ref[pl.ds(at, block), :].astype(bf16)


def kernel_c(
    place_ref, params_ref, gates_ref, q_ref, k_ref, g_ref, s_ref, u_ref, z_ref, end_ref, *refs, steps
):
    v_in = refs[:steps]
    dq_ref, dk_ref, gate_ref, small_ref, v_ref = refs[steps:]
    heads, n, hd = z_ref.shape
    me = place_ref[0]
    block = n // steps
    for m in range(steps):
        at = pl.multiple_of((me ^ m) * block, block)
        v_ref[pl.ds(at, block), :] = v_in[m][...].astype(f32)
    i, j = positions(n)
    rows, sums, sum_rows, strengths = shared(gates_ref, params_ref, heads, i, j)
    col_terms, row_terms, extra, keep = [], [], [], []
    for h in range(heads):
        cols = slice(h * hd, (h + 1) * hd)
        qraw, qinv = units(q_ref, h, hd)
        kraw, kinv = units(k_ref, h, hd)
        q = qraw * qinv * hd ** (-0.5)
        k = kraw * kinv
        last = sums[h][n - 1 : n, :]
        tail = jnp.exp(last - sums[h])
        grown = jnp.exp(sums[h])
        fade = jnp.where(i <= j, jnp.exp(jnp.where(i <= j, sum_rows[h] - sums[h], 0.0)), 0.0)
        gram = mm(k, k, 1, 1)
        cross = mm(k, q, 1, 1)
        cot = g_ref[:, cols]
        state = s_ref[h]
        end = end_ref[h]
        z = z_ref[h]
        k_state = grown * mm(k, state)
        new = mm(u_ref[h], strengths[h] * (v_ref[:, cols] - k_state), 0, 0)
        dq_in = grown * mm(cot, state, 1, 1)
        dk_in = -grown * mm(strengths[h] * z, state, 1, 1)
        near = fade * mm(new, cot, 1, 1)
        solve = jnp.where(i < j, -fade * rows[h][1] * mm(new, z, 1, 1), 0.0)
        pairs = near * cross + solve * gram
        weight = jnp.sum(new * (tail * mm(k, end)), axis=1, keepdims=True)
        own = (
            jnp.sum(q * dq_in, axis=1, keepdims=True)
            + jnp.sum(k * dk_in, axis=1, keepdims=True)
            - jnp.sum(pairs, axis=1, keepdims=True)
            - weight
        )
        total = jnp.sum(weight, axis=0, keepdims=True) + jnp.exp(last) * jnp.sum(
            jnp.sum(state * end, axis=1, keepdims=True), axis=0, keepdims=True
        )
        col_terms.append(own)
        col_terms.append(jnp.sum(z * new, axis=1, keepdims=True))
        row_terms.append(jnp.sum(pairs, axis=0, keepdims=True))
        extra.append(total)
        both = jnp.concatenate([near, solve], axis=1).astype(bf16)
        by_key = mm(both, k, 0, 0)
        dq = by_key[:n] + dq_in
        dk = (
            mm(near, q)
            + mm(solve, k)
            + by_key[n:]
            + dk_in
            + tail * mm(new, end, 1, 1)
        )
        dq = (hd ** (-0.5)) * (
            qinv * dq - qraw * (qinv * qinv * qinv * jnp.sum(qraw * dq, axis=1, keepdims=True))
        )
        dk = kinv * dk - kraw * (kinv * kinv * kinv * jnp.sum(kraw * dk, axis=1, keepdims=True))
        dq_ref[:, cols] = dq.astype(bf16)
        dk_ref[:, cols] = dk.astype(bf16)
    from_rows = to_columns(row_terms)
    strength_rows = to_rows([col_terms[2 * h + 1] for h in range(heads)])
    si = lax.broadcasted_iota(jnp.int32, small_ref.shape, 0)
    sj = lax.broadcasted_iota(jnp.int32, small_ref.shape, 1)
    small = jnp.zeros(small_ref.shape, f32)
    for h in range(heads):
        change = col_terms[2 * h] + from_rows[h]
        dlog = jnp.sum(jnp.where(i >= j, change, 0.0), axis=0, keepdims=True) + extra[h]
        dgate = dlog * rows[h][2]
        gate_ref[0, h : h + 1, :] = dgate
        gate_ref[1, h : h + 1, :] = strength_rows[h] * (1.0 - rows[h][1])
        first = jnp.sum(dlog * rows[h][0], axis=1, keepdims=True)
        second = jnp.sum(dgate, axis=1, keepdims=True)
        small = small + jnp.where((si == 0) & (sj == h), first, 0.0)
        small = small + jnp.where((si == 1) & (sj == h), second, 0.0)
    small_ref[...] = small


def kernel_values(place_ref, *refs, chips, chunks):
    tokens = refs[:chips]
    mine = refs[chips : chips + chunks]
    theirs = refs[chips + chunks : chips + 2 * chunks]
    outs = refs[chips + 2 * chunks :]
    core = place_ref[0]
    block = tokens[0].shape[0]
    part, width = mine[0].shape
    own_at = pl.multiple_of(core * part, part)
    other_at = pl.multiple_of((1 - core) * part, part)
    own = jnp.concatenate([ref[:, pl.ds(own_at, part)] for ref in tokens], axis=0)
    other = jnp.concatenate([ref[:, pl.ds(other_at, part)] for ref in tokens], axis=0)
    for m in range(chunks):
        result = jnp.dot(own, mine[m][...], preferred_element_type=f32) + jnp.dot(
            other, theirs[m][...], preferred_element_type=f32
        )
        for s in range(chips):
            outs[s][:, m * width : (m + 1) * width] = result[s * block : (s + 1) * block].astype(
                bf16
            )


def kernel_sum(*refs, chips):
    total = refs[0][...].astype(f32)
    for ref in refs[1:chips]:
        total = total + ref[...].astype(f32)
    outs = refs[chips:]
    width = outs[0].shape[1]
    for m, out_ref in enumerate(outs):
        out_ref[...] = total[:, m * width : (m + 1) * width].astype(out_ref.dtype)


def kernel_input(place_ref, *refs, chips, steps):
    grads = refs[:chips]
    mine = refs[chips : chips + steps]
    theirs = refs[chips + steps : chips + 2 * steps]
    outs = refs[chips + 2 * steps :]
    core = place_ref[0]
    block = grads[0].shape[0]
    part, width = mine[0].shape
    rows = jnp.concatenate([ref[...] for ref in grads], axis=0)
    for chunks, at in ((mine, core * part), (theirs, (1 - core) * part)):
        total = None
        for m in range(steps):
            piece = lax.dot_general(
                rows[:, m * width : (m + 1) * width],
                chunks[m][...],
                (((1,), (1,)), ((), ())),
                preferred_element_type=f32,
            )
            total = piece if total is None else total + piece
        place = pl.multiple_of(at, part)
        for s in range(chips):
            outs[s][:, pl.ds(place, part)] = total[s * block : (s + 1) * block].astype(bf16)


def kernel_assemble(place_ref, *refs):
    out_ref = refs[-1]
    width = refs[0].shape[1]
    me = place_ref[0]
    for s, ref in enumerate(refs[:-1]):
        at = pl.multiple_of((me ^ s) * width, width)
        out_ref[:, pl.ds(at, width)] = ref[...]


def struct(shape, kind):
    return jax.ShapeDtypeStruct(shape, kind)


VMEM = pl.BlockSpec(memory_space=pltpu.VMEM)
SMEM = pl.BlockSpec(memory_space=pltpu.SMEM)
ANY = pl.BlockSpec(memory_space=pl.ANY)


def call(body, args, specs, outs, name, scratch=(), out_specs=None):
    return pl.pallas_call(
        body,
        in_specs=list(specs),
        out_specs=[VMEM] * len(outs) if out_specs is None else out_specs,
        out_shape=list(outs),
        scratch_shapes=list(scratch),
        compiler_params=pltpu.CompilerParams(vmem_limit_bytes=48 * 1024 * 1024),
        name=name,
    )(*args)


def per_device(
    layer_input, value_weight, query_raw, key_raw, out_grad, gate_logits, decay_params, saved_states
):
    plane = ("dp", "ctx")
    cores = 2
    blocks = lax.axis_size("ctx")
    members = lax.axis_size("dp") * blocks
    chips = members // cores
    steps = lax.axis_size("tp")
    here = lax.axis_index("dp") * blocks + lax.axis_index("ctx")
    level_s = lax.axis_index("tp").reshape(1).astype(jnp.int32)
    chip = here // cores
    chip_s = chip.reshape(1).astype(jnp.int32)
    core_s = (here % cores).reshape(1).astype(jnp.int32)
    tokens = layer_input[0]
    block, model = tokens.shape
    part, width = value_weight.shape
    hd = saved_states.shape[-1]
    heads = query_raw.shape[2] // hd
    length = query_raw.shape[1]
    q, k, g = query_raw[0], key_raw[0], out_grad[0]
    gates = gate_logits[:, 0]
    states = saved_states[0, 0]

    def turn(array, m, places=None):
        pairs = [(t, t ^ m) for t in range(steps) if places is None or t in places]
        return lax.ppermute(array, "tp", pairs)

    def swap(array):
        return lax.ppermute(array, plane, [(p, p ^ 1) for p in range(members)])

    def cross(array, s):
        return lax.ppermute(array, plane, [(p, p ^ (cores * s)) for p in range(members)])

    mine = {0: value_weight}
    for m in sorted(range(1, steps), key=lambda m: (m // 4, (-m) % 2, m)):
        if m % 4 == 3:
            inner = [t for t in range(steps) if t % 4 in (1, 2)]
            straight = turn(value_weight, m, inner)
            relayed = turn(mine[m - 1], 1, inner)
            mine[m] = jnp.where((lax.axis_index("tp") + 1) % 4 < 2, relayed, straight)
        else:
            mine[m] = turn(value_weight, m)
    theirs = {m: swap(mine[m]) for m in range(steps)}

    bc, far, x1, z0, inverse = call(
        kernel_a,
        (gates, decay_params, q, k, g),
        (VMEM, SMEM, VMEM, VMEM, VMEM),
        (
            struct((heads, hd, 2 * hd), bf16),
            struct((heads, hd, hd), bf16),
            struct((heads, length, hd), bf16),
            struct((heads, length, hd), f32),
            struct((heads, length, length), f32),
        ),
        "maps",
    )
    received = []
    for d in range(1, blocks):
        received.append(
            lax.ppermute(
                bc if d < blocks - 1 else far, "ctx", [(p, p - d) for p in range(d, blocks)]
            )
        )

    token_parts = []
    for s in range(chips):
        piece = lax.dynamic_slice_in_dim(tokens, (chip ^ s) * (cores * part), cores * part, 1)
        token_parts.append(piece if s == 0 else cross(piece, s))

    outs = call(
        functools.partial(kernel_b, count=len(received), steps=steps),
        (level_s, gates, x1, z0, *received),
        (SMEM,) + (VMEM,) * (3 + len(received)),
        tuple(struct((block, width), bf16) for _ in range(steps))
        + (struct((heads, length, hd), f32), struct((heads, hd, hd), f32)),
        "value_grad",
        scratch=(pltpu.VMEM((length, width), f32),),
    )
    dv_blocks, z, end = outs[:steps], outs[steps], outs[steps + 1]
    dv_cols = [dv_blocks[m] if m == 0 else turn(dv_blocks[m], m) for m in range(steps)]
    dv_row = jnp.concatenate(dv_cols, axis=1)
    dv_parts = [dv_row if s == 0 else cross(dv_row, s) for s in range(chips)]

    groups = [tuple(range(steps - 1)), (steps - 1,)]
    v_blocks = []
    for group in groups:
        sums = call(
            functools.partial(kernel_values, chips=chips, chunks=len(group)),
            (core_s, *token_parts, *[mine[m] for m in group], *[theirs[m] for m in group]),
            (SMEM,) + (VMEM,) * (chips + 2 * len(group)),
            tuple(struct((block, width * len(group)), bf16) for _ in range(chips)),
            f"values{group[0]}",
        )
        back = [sums[s] if s == 0 else cross(sums[s], s) for s in range(chips)]
        whole = call(
            functools.partial(kernel_sum, chips=chips),
            tuple(back),
            (VMEM,) * chips,
            tuple(struct((block, width), bf16) for _ in group),
            f"sum{group[0]}",
        )
        v_blocks += [part_v if m == 0 else turn(part_v, m) for m, part_v in zip(group, whole)]

    in_blocks = call(
        functools.partial(kernel_input, chips=chips, steps=steps),
        (core_s, *dv_parts, *[mine[m] for m in range(steps)], *[theirs[m] for m in range(steps)]),
        (SMEM,) + (VMEM,) * (chips + 2 * steps),
        tuple(struct((block, cores * part), bf16) for _ in range(chips)),
        "input_grad",
    )
    in_back = [in_blocks[s] if s == 0 else cross(in_blocks[s], s) for s in range(chips)]
    input_grad = call(
        kernel_assemble,
        (chip_s, *in_back),
        (SMEM,) + (VMEM,) * chips,
        (struct((block, model), bf16),),
        "assemble",
    )[0]

    dq, dk, gate, small = call(
        functools.partial(kernel_c, steps=steps),
        (level_s, decay_params, gates, q, k, g, states, inverse, z, end, *v_blocks),
        (SMEM, SMEM) + (VMEM,) * (8 + steps),
        (
            struct((length, width), bf16),
            struct((length, width), bf16),
            struct((2, heads, length), f32),
            struct((8, 128), f32),
        ),
        "gradients",
        scratch=(pltpu.VMEM((length, width), f32),),
    )
    small = small + swap(small)
    shares = [small if s == 0 else cross(small, s) for s in range(chips)]
    decay_grad = sum(shares[1:], shares[0])[:2, :heads]
    return (input_grad[None], dq[None], dk[None], gate[:, None], decay_grad)


def solution(mesh):
    placed = (
        P("dp", ("ctx", "tp"), None),
        P(("dp", "ctx"), "tp"),
        P("dp", "ctx", "tp"),
        P("dp", "ctx", "tp"),
        P("dp", "ctx", "tp"),
        P(None, "dp", "tp", "ctx"),
        P(None, "tp"),
        P("dp", "ctx", "tp", None, None),
    )
    return jax.shard_map(
        per_device,
        mesh=mesh,
        in_specs=placed,
        out_specs=(
            P("dp", ("ctx", "tp"), None),
            P("dp", "ctx", "tp"),
            P("dp", "ctx", "tp"),
            P(None, "dp", "tp", "ctx"),
            P(None, "tp"),
        ),
        check_vma=False,
    )
```

```python
import functools
import jax
import jax.numpy as jnp
from jax import lax
from jax.experimental import pallas as pl
from jax.experimental.pallas import tpu as pltpu
from jax.sharding import PartitionSpec as P


f32 = jnp.float32
bf16 = jnp.bfloat16
epsilon = 1e-06
BASE = 8
LOW = 64


def place_core():
    return lax.axis_index("ctx") & 1


def place_chip():
    return lax.axis_index("dp") * (lax.axis_size("ctx") // 2) + (lax.axis_index("ctx") >> 1)


def place_level():
    return lax.axis_index("tp")


def mm(a, b, ca=1, cb=0):
    return lax.dot_general(
        a.astype(bf16), b.astype(bf16), (((ca,), (cb,)), ((), ())), preferred_element_type=f32
    )


def halves(a):
    high = a.astype(bf16)
    return high, (a - high.astype(f32)).astype(bf16)


def mm3(a, b, ca=1, cb=0):
    ah, al = halves(a)
    bh, bl = halves(b)
    return mm(ah, bh, ca, cb) + (mm(ah, bl, ca, cb) + mm(al, bh, ca, cb))


def softplus(x):
    return jnp.maximum(x, 0.0) + jnp.log(1.0 + jnp.exp(-jnp.abs(x)))


def sigmoid(x):
    return 1.0 / (1.0 + jnp.exp(-x))


def positions(n):
    return (
        lax.broadcasted_iota(jnp.int32, (n, n), 0),
        lax.broadcasted_iota(jnp.int32, (n, n), 1),
    )


def stack_rows(rows):
    n = rows[0].shape[1]
    short = -len(rows) % 8
    return jnp.concatenate(list(rows) + [jnp.zeros((1, n), f32)] * short, axis=0)


def to_columns(rows):
    turned = stack_rows(rows).T
    return [turned[:, i : i + 1] for i in range(len(rows))]


def to_rows(columns):
    n = columns[0].shape[0]
    short = -len(columns) % 8
    turned = jnp.concatenate(list(columns) + [jnp.zeros((n, 1), f32)] * short, axis=1).T
    return [turned[i : i + 1] for i in range(len(columns))]


def gate_rows(gates_ref, params_ref, heads):
    out = []
    for h in range(heads):
        ga = gates_ref[0, h : h + 1, :]
        gb = gates_ref[1, h : h + 1, :]
        scale = jnp.exp(jnp.broadcast_to(params_ref[0:1, h : h + 1], ga.shape))
        shifted = ga + params_ref[1:2, h : h + 1]
        out.append((-scale * softplus(shifted), sigmoid(gb), -scale * sigmoid(shifted)))
    return out


def cumulated(logs, i, j):
    return [jnp.sum(jnp.where(j <= i, row, 0.0), axis=1, keepdims=True) for row in logs]


def thirds(ref):
    n = ref.shape[0] // 3
    return [ref.at[index * n : (index + 1) * n] for index in range(3)]


def units(ref, h, hd):
    raw = ref[:, h * hd : (h + 1) * hd].astype(f32)
    inv = lax.rsqrt(jnp.sum(raw * raw, axis=-1, keepdims=True) + epsilon)
    return raw, inv


def folded(a, i, j, size):
    a = jnp.where((i ^ j) < size, a, 0.0)
    return functools.reduce(jnp.add, [a[g : g + size] for g in range(0, a.shape[0], size)])


def dot_blocks(a, b, keep):
    def spread(part):
        return jnp.concatenate([part] * (part.shape[1] // part.shape[0]), axis=0) * keep

    ah, al = halves(a)
    bh, bl = [spread(part) for part in halves(b)]
    return mm(ah, bh) + (mm(ah, bl) + mm(al, bh))


def inverse_upper(strict, i, j):
    n = strict[0].shape[0]
    size = min(LOW, n)

    def frame(size):
        r = lax.broadcasted_iota(jnp.int32, (size, n), 0)
        c = lax.broadcasted_iota(jnp.int32, (size, n), 1) & (size - 1)
        keep = ((i ^ j) < size).astype(f32).astype(bf16)
        return r ^ c, keep, [folded(a, i, j, size) for a in strict]

    apart, keep, parts = frame(size)
    power = [jnp.where(apart < BASE, a, 0.0) for a in parts]
    result = [(apart == 0).astype(f32) - a for a in power]
    k = 2
    while k < BASE:
        power = [dot_blocks(a, a, keep) for a in power]
        result = [u + dot_blocks(u, a, keep) for u, a in zip(result, power)]
        k *= 2
    b = BASE
    while 2 * b < n:
        if 2 * b > size:
            size = 2 * b
            apart, keep, parts = frame(size)
            result = [
                jnp.where(apart < b, jnp.concatenate([u, u], axis=0), 0.0) for u in result
            ]
        cross = (apart < 2 * b) & (apart >= b)
        part = [dot_blocks(u, jnp.where(cross, a, 0.0), keep) for u, a in zip(result, parts)]
        result = [u - dot_blocks(x, u, keep) for u, x in zip(result, part)]
        b *= 2
    out = []
    part = [mm3(u[:, :b], a[:b, b:]) for u, a in zip(result, strict)]
    part = [mm3(x, u[:, b:]) for u, x in zip(result, part)]
    for u, x in zip(result, part):
        top = jnp.concatenate([u[:, :b], -x], axis=1)
        low = jnp.concatenate([jnp.zeros((b, b), f32), u[:, b:]], axis=1)
        out.append(jnp.concatenate([top, low], axis=0))
    return out


def shared(gates_ref, params_ref, heads, i, j):
    rows = gate_rows(gates_ref, params_ref, heads)
    sums = cumulated([r[0] for r in rows], i, j)
    sum_rows = to_rows(sums)
    strength_cols = to_columns([r[1] for r in rows])
    return rows, sums, sum_rows, strength_cols


def kernel_a(gates_ref, params_ref, tokens_ref, bc_ref, x_ref, z_ref, u_ref):
    q_ref, k_ref, g_ref = thirds(tokens_ref)
    heads, hd = bc_ref.shape[0], bc_ref.shape[1]
    n = q_ref.shape[0]
    i, j = positions(n)
    rows, sums, sum_rows, strengths = shared(gates_ref, params_ref, heads, i, j)
    strict, scores, ks, qs = [], [], [], []
    for h in range(heads):
        qraw, qinv = units(q_ref, h, hd)
        kraw, kinv = units(k_ref, h, hd)
        q = qraw * qinv * hd ** (-0.5)
        k = kraw * kinv
        fade = jnp.where(i <= j, jnp.exp(jnp.where(i <= j, sum_rows[h] - sums[h], 0.0)), 0.0)
        strict.append(jnp.where(i < j, fade * rows[h][1] * mm(k, k, 1, 1), 0.0))
        scores.append(fade * mm(k, q, 1, 1))
        ks.append(k)
        qs.append(q)
    inverse = inverse_upper(strict, i, j)
    ei, ej = positions(hd)
    for h in range(heads):
        last = sums[h][n - 1 : n, :]
        tail = jnp.exp(last - sums[h])
        grown = jnp.exp(sums[h])
        cot = g_ref[:, h * hd : (h + 1) * hd]
        right = jnp.concatenate([ks[h] * tail, mm(scores[h], cot)], axis=1)
        x = mm(inverse[h], right)
        y = mm(strengths[h] * grown * ks[h], x, 0, 0)
        b = jnp.where(ei == ej, jnp.exp(last), 0.0) - y[:, :hd]
        c = mm(qs[h] * grown, cot, 0, 0) - y[:, hd:]
        bc_ref[h] = jnp.concatenate([b, c], axis=1).astype(bf16)
        x_ref[h] = x[:, :hd].astype(bf16)
        z_ref[h] = x[:, hd:]
        u_ref[h] = inverse[h]


def kernel_compose(bc_ref, other_ref, *outs, full):
    heads, hd = bc_ref.shape[0], bc_ref.shape[1]
    first = jnp.full((hd, 2 * hd), place_core(), jnp.int32) == 0
    for h in range(heads):
        a = bc_ref[h].astype(f32)
        b = other_ref[h].astype(f32)
        early = jnp.where(first, a, b)
        late = jnp.where(first, b, a)
        joined = mm(early[:, :hd], late if full else late[:, hd:])
        c = joined[:, -hd:] + early[:, hd:]
        outs[0][h] = c.astype(bf16)
        if full:
            outs[1][h] = jnp.concatenate([joined[:, :hd], c], axis=1).astype(bf16)


def kernel_b(gates_ref, x_ref, z0_ref, other_ref, *refs, count, steps):
    received = refs[:count]
    outs = refs[count : count + steps]
    z_ref, end_ref, dv_ref = refs[count + steps :]
    heads, n, hd = x_ref.shape
    me = place_level()
    last = jnp.full((hd, hd), place_core(), jnp.int32) == 1
    strengths = to_columns([sigmoid(gates_ref[1, h : h + 1, :]) for h in range(heads)])
    for h in range(heads):
        end = jnp.zeros((hd, hd), f32)
        for index, ref in reversed(list(enumerate(received))):
            if index == count - 1:
                end = ref[h].astype(f32)
            else:
                end = mm(ref[h, :, :hd], end) + ref[h, :, hd:].astype(f32)
        inner = mm(other_ref[h, :, :hd], end) + other_ref[h, :, hd:].astype(f32)
        end = jnp.where(last, end, inner)
        z = z0_ref[h] + mm(x_ref[h], end)
        z_ref[h] = z
        end_ref[h] = end
        dv_ref[:, h * hd : (h + 1) * hd] = strengths[h] * z
    block = n // steps
    for m in range(steps):
        at = pl.multiple_of((me ^ m) * block, block)
        outs[m][...] = dv_ref[pl.ds(at, block), :].astype(bf16)


def kernel_pre(
    gates_ref,
    params_ref,
    tokens_ref,
    s_ref,
    u_ref,
    z_ref,
    end_ref,
    ut_ref,
    fade_ref,
    sink_ref,
    gram_ref,
    cross_ref,
    ks_ref,
    qn_ref,
    kn_ref,
    dq_ref,
    dk_ref,
    kend_ref,
    side_ref,
):
    q_ref, k_ref, g_ref = thirds(tokens_ref)
    heads, n, hd = z_ref.shape
    i, j = positions(n)
    rows, sums, sum_rows, strengths = shared(gates_ref, params_ref, heads, i, j)
    sides = []
    for h in range(heads):
        qraw, qinv = units(q_ref, h, hd)
        kraw, kinv = units(k_ref, h, hd)
        q = qraw * qinv * hd ** (-0.5)
        k = kraw * kinv
        last = sums[h][n - 1 : n, :]
        tail = jnp.exp(last - sums[h])
        grown = jnp.exp(sums[h])
        fade = jnp.where(i <= j, jnp.exp(jnp.where(i <= j, sum_rows[h] - sums[h], 0.0)), 0.0)
        state = s_ref[h]
        end = end_ref[h]
        ut_ref[h] = u_ref[h].T.astype(bf16)
        fade_ref[h] = fade
        sink_ref[h] = jnp.where(i < j, -fade * rows[h][1], 0.0)
        gram_ref[h] = mm(k, k, 1, 1)
        cross_ref[h] = mm(k, q, 1, 1)
        ks_ref[h] = grown * mm(k, state)
        qn_ref[h] = q.astype(bf16)
        kn_ref[h] = k.astype(bf16)
        dq_in = grown * mm(g_ref[:, h * hd : (h + 1) * hd], state, 1, 1)
        dk_in = -grown * mm(strengths[h] * z_ref[h], state, 1, 1)
        dq_ref[h] = dq_in
        dk_ref[h] = dk_in
        kend_ref[h] = tail * mm(k, end)
        sides.append(
            jnp.sum(q * dq_in, axis=1, keepdims=True) + jnp.sum(k * dk_in, axis=1, keepdims=True)
        )
        sides.append(tail)
        sides.append(strengths[h])
        total = jnp.exp(last) * jnp.sum(
            jnp.sum(state * end, axis=1, keepdims=True), axis=0, keepdims=True
        )
        sides.append(jnp.broadcast_to(total, (n, 1)))
    side_ref[...] = jnp.concatenate(sides, axis=1)


def kernel_gates(
    gates_ref,
    params_ref,
    tokens_ref,
    z_ref,
    ut_ref,
    fade_ref,
    sink_ref,
    gram_ref,
    cross_ref,
    ks_ref,
    kend_ref,
    side_ref,
    *refs,
    steps,
):
    g_ref = thirds(tokens_ref)[2]
    v_in = refs[:steps]
    gate_ref, small_ref, both_ref, new_ref, v_ref = refs[steps:]
    heads, n, hd = z_ref.shape
    me = place_level()
    block = n // steps
    for m in range(steps):
        at = pl.multiple_of((me ^ m) * block, block)
        v_ref[pl.ds(at, block), :] = v_in[m][...].astype(f32)
    i, j = positions(n)
    rows = gate_rows(gates_ref, params_ref, heads)
    side = side_ref[...]
    changes, products, sums, extra = [], [], [], []
    for h in range(heads):
        cols = slice(h * hd, (h + 1) * hd)
        base = side[:, 4 * h : 4 * h + 1]
        strength = side[:, 4 * h + 2 : 4 * h + 3]
        z = z_ref[h]
        new = mm(ut_ref[h], strength * (v_ref[:, cols] - ks_ref[h]))
        near = fade_ref[h] * mm(new, g_ref[:, cols], 1, 1)
        solve = sink_ref[h] * mm(new, z, 1, 1)
        both_ref[h, :, :n] = near.astype(bf16)
        both_ref[h, :, n:] = solve.astype(bf16)
        new_ref[h] = new.astype(bf16)
        pairs = near * cross_ref[h] + solve * gram_ref[h]
        weight = jnp.sum(new * kend_ref[h], axis=1, keepdims=True)
        changes.append(base - jnp.sum(pairs, axis=1, keepdims=True) - weight)
        products.append(jnp.sum(z * new, axis=1, keepdims=True))
        sums.append(jnp.sum(pairs, axis=0, keepdims=True))
        extra.append(jnp.sum(weight, axis=0, keepdims=True) + side[0:1, 4 * h + 3 : 4 * h + 4])
    from_rows = to_columns(sums)
    strength_rows = to_rows(products)
    si = lax.broadcasted_iota(jnp.int32, small_ref.shape, 0)
    sj = lax.broadcasted_iota(jnp.int32, small_ref.shape, 1)
    small = jnp.zeros(small_ref.shape, f32)
    for h in range(heads):
        change = changes[h] + from_rows[h]
        dlog = jnp.sum(jnp.where(i >= j, change, 0.0), axis=0, keepdims=True) + extra[h]
        dgate = dlog * rows[h][2]
        gate_ref[0, h : h + 1, :] = dgate
        gate_ref[1, h : h + 1, :] = strength_rows[h] * (1.0 - rows[h][1])
        first = jnp.sum(dlog * rows[h][0], axis=1, keepdims=True)
        second = jnp.sum(dgate, axis=1, keepdims=True)
        small = small + jnp.where((si == 0) & (sj == h), first, 0.0)
        small = small + jnp.where((si == 1) & (sj == h), second, 0.0)
    small_ref[...] = small


def kernel_units(
    tokens_ref, qn_ref, kn_ref, end_ref, dq_in_ref, dk_in_ref, side_ref, both_ref, new_ref, *outs
):
    dq_ref, dk_ref = outs
    q_ref, k_ref, _ = thirds(tokens_ref)
    heads, n, hd = new_ref.shape
    side = side_ref[...]
    for h in range(heads):
        cols = slice(h * hd, (h + 1) * hd)
        qraw, qinv = units(q_ref, h, hd)
        kraw, kinv = units(k_ref, h, hd)
        tail = side[:, 4 * h + 1 : 4 * h + 2]
        both = both_ref[h]
        by_key = mm(both, kn_ref[h], 0, 0)
        dq = by_key[:n] + dq_in_ref[h]
        dk = (
            mm(both[:, :n], qn_ref[h])
            + mm(both[:, n:], kn_ref[h])
            + by_key[n:]
            + dk_in_ref[h]
            + tail * mm(new_ref[h], end_ref[h], 1, 1)
        )
        dq = (hd ** (-0.5)) * (
            qinv * dq - qraw * (qinv * qinv * qinv * jnp.sum(qraw * dq, axis=1, keepdims=True))
        )
        dk = kinv * dk - kraw * (kinv * kinv * kinv * jnp.sum(kraw * dk, axis=1, keepdims=True))
        dq_ref[:, cols] = dq.astype(bf16)
        dk_ref[:, cols] = dk.astype(bf16)


def pieces(group):
    return sum(2 if m % 4 == 3 else 1 for m in group)


def pick(level, m, refs, scratch):
    if m % 4 != 3:
        return refs.pop(0)[...]
    straight, relayed = refs.pop(0), refs.pop(0)
    outer = (level + 1) % 4 < 2

    @pl.when(outer)
    def _():
        scratch[...] = relayed[...]

    @pl.when(jnp.logical_not(outer))
    def _():
        scratch[...] = straight[...]

    return scratch[...]


def kernel_values(*refs, chips, group):
    tokens = refs[:chips]
    chunks = pieces(group)
    mine = list(refs[chips : chips + chunks])
    theirs = list(refs[chips + chunks : chips + 2 * chunks])
    outs = refs[chips + 2 * chunks : -1]
    scratch = refs[-1]
    core = place_core()
    level = place_level()
    block = tokens[0].shape[0]
    part, width = mine[0].shape
    own_at = pl.multiple_of(core * part, part)
    other_at = pl.multiple_of((1 - core) * part, part)
    own = jnp.concatenate([ref[:, pl.ds(own_at, part)] for ref in tokens], axis=0)
    other = jnp.concatenate([ref[:, pl.ds(other_at, part)] for ref in tokens], axis=0)
    for m, number in enumerate(group):
        result = jnp.dot(
            own, pick(level, number, mine, scratch.at[0]), preferred_element_type=f32
        ) + jnp.dot(other, pick(level, number, theirs, scratch.at[1]), preferred_element_type=f32)
        for s in range(chips):
            outs[s][:, m * width : (m + 1) * width] = result[s * block : (s + 1) * block].astype(
                bf16
            )


def kernel_cut(tokens_hbm, *refs):
    outs, sems = refs[:-1], refs[-1]
    width = outs[0].shape[1]
    copies = []
    for s, out in enumerate(outs):
        at = pl.multiple_of((place_chip() ^ s) * width, width)
        copies.append(pltpu.make_async_copy(tokens_hbm.at[:, pl.ds(at, width)], out, sems.at[s]))
    for copy in copies:
        copy.start()
    for copy in copies:
        copy.wait()


def kernel_sum(*refs, chips):
    total = refs[0][...].astype(f32)
    for ref in refs[1:chips]:
        total = total + ref[...].astype(f32)
    outs = refs[chips:]
    width = outs[0].shape[1]
    for m, out_ref in enumerate(outs):
        out_ref[...] = total[:, m * width : (m + 1) * width].astype(out_ref.dtype)


def kernel_input(*refs, chips, group, first, final):
    grads = refs[:chips]
    chunks = pieces(group)
    mine = list(refs[chips : chips + chunks])
    theirs = list(refs[chips + chunks : chips + 2 * chunks])
    rest = list(refs[chips + 2 * chunks :])
    before = None if first else rest.pop(0)
    scratch = rest.pop()
    core = place_core()
    level = place_level()
    block = grads[0].shape[0]
    part, width = mine[0].shape
    rows = jnp.concatenate([ref[...] for ref in grads], axis=0)
    for index, (found, at) in enumerate(((mine, core * part), (theirs, (1 - core) * part))):
        total = None if first else before[index]
        for m in group:
            piece = lax.dot_general(
                rows[:, m * width : (m + 1) * width],
                pick(level, m, found, scratch.at[index]),
                (((1,), (1,)), ((), ())),
                preferred_element_type=f32,
            )
            total = piece if total is None else total + piece
        if final:
            place = pl.multiple_of(at, part)
            for s in range(chips):
                rest[s][:, pl.ds(place, part)] = total[s * block : (s + 1) * block].astype(bf16)
        else:
            rest[0][index] = total


def kernel_assemble(*refs):
    out_ref = refs[-1]
    width = refs[0].shape[1]
    me = place_chip()
    for s, ref in enumerate(refs[:-1]):
        at = pl.multiple_of((me ^ s) * width, width)
        out_ref[:, pl.ds(at, width)] = ref[...]


def kernel_join(*refs):
    out_ref = refs[-1]
    width = refs[0].shape[1]
    for m, ref in enumerate(refs[:-1]):
        out_ref[:, m * width : (m + 1) * width] = ref[...]


def kernel_decay(*refs):
    out_ref = refs[-1]
    total = functools.reduce(jnp.add, [ref[...] for ref in refs[:-1]])
    out_ref[...] = total[: out_ref.shape[0], : out_ref.shape[1]]


def struct(shape, kind):
    return jax.ShapeDtypeStruct(shape, kind)


VMEM = pl.BlockSpec(memory_space=pltpu.VMEM)
HBM = pl.BlockSpec(memory_space=pltpu.HBM)


def call(body, args, specs, outs, scratch=(), loads=()):
    specs = list(specs)
    grid = {}
    if loads:
        grid = dict(grid=(1,))
        for index in loads:
            shape = args[index].shape
            specs[index] = pl.BlockSpec(shape, lambda i, rank=len(shape): (0,) * rank)
    return pl.pallas_call(
        body,
        in_specs=specs,
        out_specs=[VMEM] * len(outs),
        out_shape=list(outs),
        scratch_shapes=list(scratch),
        cost_estimate=pl.CostEstimate(
            flops=3 * 10**9, bytes_accessed=20 * 10**6, transcendentals=0
        ),
        compiler_params=pltpu.CompilerParams(vmem_limit_bytes=12 * 1024 * 1024),
        **grid,
    )(*args)


def weight_order(steps):
    return sorted(range(1, steps), key=lambda m: (m // 4, (-m) % 2, m))


def per_device(
    layer_input, value_weight, query_raw, key_raw, out_grad, gate_logits, decay_params, saved_states
):
    plane = ("dp", "ctx")
    cores = 2
    blocks = lax.axis_size("ctx")
    members = lax.axis_size("dp") * blocks
    chips = members // cores
    steps = lax.axis_size("tp")
    tokens = layer_input[0]
    block, model = tokens.shape
    part, width = value_weight.shape
    hd = saved_states.shape[-1]
    heads = query_raw.shape[2] // hd
    length = query_raw.shape[1]
    q, k, g = query_raw[0], key_raw[0], out_grad[0]
    gates = gate_logits[:, 0]
    stacked = jnp.concatenate([q, k, g])
    states = saved_states[0, 0]

    def turn(array, m, places=None):
        pairs = [(t, t ^ m) for t in range(steps) if places is None or t in places]
        return lax.ppermute(array, "tp", pairs)

    def swap(array):
        return lax.ppermute(array, plane, [(p, p ^ 1) for p in range(members)])

    def cross(array, s):
        return lax.ppermute(array, plane, [(p, p ^ (cores * s)) for p in range(members)])

    mine = {0: (value_weight,)}
    for m in weight_order(steps):
        if m % 4 == 3:
            inner = [t for t in range(steps) if t % 4 in (1, 2)]
            straight = turn(value_weight, m, inner)
            relayed = turn(mine[m - 1][0], 1, inner)
            mine[m] = (straight, relayed)
        else:
            mine[m] = (turn(value_weight, m),)
    theirs = {m: tuple(swap(a) for a in mine[m]) for m in range(steps)}

    def chunks(found, group):
        return [a for m in group for a in found[m]]

    bc, x1, z0, inverse = call(
        kernel_a,
        (gates, decay_params, stacked),
        (VMEM, VMEM, VMEM),
        (
            struct((heads, hd, 2 * hd), bf16),
            struct((heads, length, hd), bf16),
            struct((heads, length, hd), f32),
            struct((heads, length, length), f32),
        ),
    )
    other = swap(bc)
    ranks = blocks // cores
    full = ranks > 2
    joined = call(
        functools.partial(kernel_compose, full=full),
        (bc, other),
        (VMEM, VMEM),
        (struct((heads, hd, hd), bf16),) + ((struct((heads, hd, 2 * hd), bf16),) if full else ()),
    )
    received = []
    for d in range(1, ranks):
        received.append(
            lax.ppermute(
                joined[1] if d < ranks - 1 else joined[0],
                "ctx",
                [(p, p - cores * d) for p in range(cores * d, blocks)],
            )
        )

    cuts = call(
        kernel_cut,
        (tokens,),
        (HBM,),
        tuple(struct((block, cores * part), bf16) for _ in range(chips)),
        scratch=(pltpu.SemaphoreType.DMA((chips,)),),
    )
    token_parts = [cuts[s] if s == 0 else cross(cuts[s], s) for s in range(chips)]

    outs = call(
        functools.partial(kernel_b, count=len(received), steps=steps),
        (gates, x1, z0, other, *received),
        (VMEM,) * (4 + len(received)),
        tuple(struct((block, width), bf16) for _ in range(steps))
        + (struct((heads, length, hd), f32), struct((heads, hd, hd), f32)),
        scratch=(pltpu.VMEM((length, width), f32),),
    )
    dv_blocks, z, end = outs[:steps], outs[steps], outs[steps + 1]
    dv_cols = [dv_blocks[m] if m == 0 else turn(dv_blocks[m], m) for m in range(steps)]
    dv_row = call(
        kernel_join, tuple(dv_cols), (VMEM,) * steps, (struct((block, steps * width), bf16),)
    )[0]
    dv_parts = [dv_row if s == 0 else cross(dv_row, s) for s in range(chips)]

    groups = [tuple(range(steps - 1)), (steps - 1,)]
    v_blocks = []
    for group in groups:
        sums = call(
            functools.partial(kernel_values, chips=chips, group=group),
            (*token_parts, *chunks(mine, group), *chunks(theirs, group)),
            (VMEM,) * (chips + 2 * len(chunks(mine, group))),
            tuple(struct((block, width * len(group)), bf16) for _ in range(chips)),
            scratch=(pltpu.VMEM((2, part, width), bf16),),
        )
        back = [sums[s] if s == 0 else cross(sums[s], s) for s in range(chips)]
        whole = call(
            functools.partial(kernel_sum, chips=chips),
            tuple(back),
            (VMEM,) * chips,
            tuple(struct((block, width), bf16) for _ in group),
        )
        v_blocks += [part_v if m == 0 else turn(part_v, m) for m, part_v in zip(group, whole)]

    acc = None
    for group in groups:
        first, final = group is groups[0], group is groups[-1]
        args = (*dv_parts, *chunks(mine, group), *chunks(theirs, group)) + (
            () if first else (acc,)
        )
        res = call(
            functools.partial(kernel_input, chips=chips, group=group, first=first, final=final),
            args,
            (VMEM,) * len(args),
            tuple(struct((block, cores * part), bf16) for _ in range(chips))
            if final
            else (struct((cores, chips * block, part), f32),),
            scratch=(pltpu.VMEM((2, part, width), bf16),),
        )
        if final:
            in_blocks = res
        else:
            acc = res[0]
    in_back = [in_blocks[s] if s == 0 else cross(in_blocks[s], s) for s in range(chips)]
    square = struct((heads, length, length), f32)
    tall = struct((heads, length, hd), f32)
    tall_half = struct((heads, length, hd), bf16)
    ut, fade, sink, gram, cross_prod, k_state, qn, kn, dq_in, dk_in, k_end, side = call(
        kernel_pre,
        (gates, decay_params, stacked, states, inverse, z, end),
        (VMEM,) * 7,
        (
            struct((heads, length, length), bf16),
            square,
            square,
            square,
            square,
            tall,
            tall_half,
            tall_half,
            tall,
            tall,
            tall,
            struct((length, 4 * heads), f32),
        ),
    )
    gate, small, both, new = call(
        functools.partial(kernel_gates, steps=steps),
        (
            gates,
            decay_params,
            stacked,
            z,
            ut,
            fade,
            sink,
            gram,
            cross_prod,
            k_state,
            k_end,
            side,
            *v_blocks,
        ),
        (VMEM,) * (12 + steps),
        (
            struct((2, heads, length), f32),
            struct((8, 128), f32),
            struct((heads, length, 2 * length), bf16),
            tall_half,
        ),
        scratch=(pltpu.VMEM((length, width), f32),),
    )
    dq, dk = call(
        kernel_units,
        (stacked, qn, kn, end, dq_in, dk_in, side, both, new),
        (VMEM,) * 9,
        (struct((length, width), bf16), struct((length, width), bf16)),
    )
    tile = (struct(small.shape, f32),)
    small = call(kernel_decay, (small, swap(small)), (VMEM, VMEM), tile)[0]
    input_grad = call(
        kernel_assemble, tuple(in_back), (VMEM,) * chips, (struct((block, model), bf16),)
    )[0]
    shares = [small if s == 0 else cross(small, s) for s in range(chips)]
    decay_grad = call(kernel_decay, tuple(shares), (VMEM,) * chips, (struct((2, heads), f32),))[0]
    return (input_grad[None], dq[None], dk[None], gate[:, None], decay_grad)


def solution(mesh):
    placed = (
        P("dp", ("ctx", "tp"), None),
        P(("dp", "ctx"), "tp"),
        P("dp", "ctx", "tp"),
        P("dp", "ctx", "tp"),
        P("dp", "ctx", "tp"),
        P(None, "dp", "tp", "ctx"),
        P(None, "tp"),
        P("dp", "ctx", "tp", None, None),
    )
    return jax.shard_map(
        per_device,
        mesh=mesh,
        in_specs=placed,
        out_specs=(
            P("dp", ("ctx", "tp"), None),
            P("dp", "ctx", "tp"),
            P("dp", "ctx", "tp"),
            P(None, "dp", "tp", "ctx"),
            P(None, "tp"),
        ),
        check_vma=False,
    )
```

```python
import functools
import jax
import jax.numpy as jnp
from jax import lax
from jax.experimental import pallas as pl
from jax.experimental.pallas import tpu as pltpu
from jax.sharding import PartitionSpec as P


f32 = jnp.float32
bf16 = jnp.bfloat16
epsilon = 1e-06
BASE = 8
LOW = 64


def place_core():
    return lax.axis_index("ctx") & 1


def place_chip():
    return lax.axis_index("dp") * (lax.axis_size("ctx") // 2) + (lax.axis_index("ctx") >> 1)


def place_level():
    return lax.axis_index("tp")


def mm(a, b, ca=1, cb=0):
    return lax.dot_general(
        a.astype(bf16), b.astype(bf16), (((ca,), (cb,)), ((), ())), preferred_element_type=f32
    )


def halves(a):
    high = a.astype(bf16)
    return high, (a - high.astype(f32)).astype(bf16)


def mm3(a, b, ca=1, cb=0):
    ah, al = halves(a)
    bh, bl = halves(b)
    return mm(ah, bh, ca, cb) + (mm(ah, bl, ca, cb) + mm(al, bh, ca, cb))


def softplus(x):
    return jnp.maximum(x, 0.0) + jnp.log1p(jnp.exp(-jnp.abs(x)))


def sigmoid(x):
    return 1.0 / (1.0 + jnp.exp(-x))


def positions(n):
    return (
        lax.broadcasted_iota(jnp.int32, (n, n), 0),
        lax.broadcasted_iota(jnp.int32, (n, n), 1),
    )


def stack_rows(rows):
    n = rows[0].shape[1]
    short = -len(rows) % 8
    return jnp.concatenate(list(rows) + [jnp.zeros((1, n), f32)] * short, axis=0)


def to_columns(rows):
    turned = stack_rows(rows).T
    return [turned[:, i : i + 1] for i in range(len(rows))]


def to_rows(columns):
    n = columns[0].shape[0]
    short = -len(columns) % 8
    turned = jnp.concatenate(list(columns) + [jnp.zeros((n, 1), f32)] * short, axis=1).T
    return [turned[i : i + 1] for i in range(len(columns))]


def gate_rows(gates_ref, params_ref, heads):
    out = []
    for h in range(heads):
        ga = gates_ref[0, h : h + 1, :]
        gb = gates_ref[1, h : h + 1, :]
        scale = jnp.exp(jnp.broadcast_to(params_ref[0:1, h : h + 1], ga.shape))
        shifted = ga + params_ref[1:2, h : h + 1]
        out.append((-scale * softplus(shifted), sigmoid(gb), -scale * sigmoid(shifted)))
    return out


def cumulated(logs, i, j):
    return [jnp.sum(jnp.where(j <= i, row, 0.0), axis=1, keepdims=True) for row in logs]


def thirds(ref):
    n = ref.shape[0] // 3
    return [ref.at[index * n : (index + 1) * n] for index in range(3)]


def units(ref, h, hd):
    raw = ref[:, h * hd : (h + 1) * hd].astype(f32)
    inv = lax.rsqrt(jnp.sum(raw * raw, axis=-1, keepdims=True) + epsilon)
    return raw, inv


def folded(a, i, j, size):
    a = jnp.where((i ^ j) < size, a, 0.0)
    return functools.reduce(jnp.add, [a[g : g + size] for g in range(0, a.shape[0], size)])


def dot_blocks(a, b, keep):
    def spread(part):
        return jnp.concatenate([part] * (part.shape[1] // part.shape[0]), axis=0) * keep

    ah, al = halves(a)
    bh, bl = [spread(part) for part in halves(b)]
    return mm(ah, bh) + (mm(ah, bl) + mm(al, bh))


def inverse_upper(strict, i, j):
    n = strict[0].shape[0]
    size = min(LOW, n)

    def frame(size):
        r = lax.broadcasted_iota(jnp.int32, (size, n), 0)
        c = lax.broadcasted_iota(jnp.int32, (size, n), 1) & (size - 1)
        keep = ((i ^ j) < size).astype(f32).astype(bf16)
        return r ^ c, keep, [folded(a, i, j, size) for a in strict]

    apart, keep, parts = frame(size)
    power = [jnp.where(apart < BASE, a, 0.0) for a in parts]
    result = [(apart == 0).astype(f32) - a for a in power]
    k = 2
    while k < BASE:
        power = [dot_blocks(a, a, keep) for a in power]
        result = [u + dot_blocks(u, a, keep) for u, a in zip(result, power)]
        k *= 2
    b = BASE
    while 2 * b < n:
        if 2 * b > size:
            size = 2 * b
            apart, keep, parts = frame(size)
            result = [
                jnp.where(apart < b, jnp.concatenate([u, u], axis=0), 0.0) for u in result
            ]
        cross = (apart < 2 * b) & (apart >= b)
        part = [dot_blocks(u, jnp.where(cross, a, 0.0), keep) for u, a in zip(result, parts)]
        result = [u - dot_blocks(x, u, keep) for u, x in zip(result, part)]
        b *= 2
    out = []
    part = [mm3(u[:, :b], a[:b, b:]) for u, a in zip(result, strict)]
    part = [mm3(x, u[:, b:]) for u, x in zip(result, part)]
    for u, x in zip(result, part):
        top = jnp.concatenate([u[:, :b], -x], axis=1)
        low = jnp.concatenate([jnp.zeros((b, b), f32), u[:, b:]], axis=1)
        out.append(jnp.concatenate([top, low], axis=0))
    return out


def shared(gates_ref, params_ref, heads, i, j):
    rows = gate_rows(gates_ref, params_ref, heads)
    sums = cumulated([r[0] for r in rows], i, j)
    sum_rows = to_rows(sums)
    strength_cols = to_columns([r[1] for r in rows])
    return rows, sums, sum_rows, strength_cols


def kernel_a(gates_ref, params_ref, tokens_ref, bc_ref, x_ref, z_ref, u_ref):
    q_ref, k_ref, g_ref = thirds(tokens_ref)
    heads, hd = bc_ref.shape[0], bc_ref.shape[1]
    n = q_ref.shape[0]
    i, j = positions(n)
    rows, sums, sum_rows, strengths = shared(gates_ref, params_ref, heads, i, j)
    strict, scores, ks, qs = [], [], [], []
    for h in range(heads):
        qraw, qinv = units(q_ref, h, hd)
        kraw, kinv = units(k_ref, h, hd)
        q = qraw * qinv * hd ** (-0.5)
        k = kraw * kinv
        fade = jnp.where(i <= j, jnp.exp(jnp.where(i <= j, sum_rows[h] - sums[h], 0.0)), 0.0)
        strict.append(jnp.where(i < j, fade * rows[h][1] * mm(k, k, 1, 1), 0.0))
        scores.append(fade * mm(k, q, 1, 1))
        ks.append(k)
        qs.append(q)
    inverse = inverse_upper(strict, i, j)
    ei, ej = positions(hd)
    for h in range(heads):
        last = sums[h][n - 1 : n, :]
        tail = jnp.exp(last - sums[h])
        grown = jnp.exp(sums[h])
        cot = g_ref[:, h * hd : (h + 1) * hd]
        right = jnp.concatenate([ks[h] * tail, mm(scores[h], cot)], axis=1)
        x = mm(inverse[h], right)
        y = mm(strengths[h] * grown * ks[h], x, 0, 0)
        b = jnp.where(ei == ej, jnp.exp(last), 0.0) - y[:, :hd]
        c = mm(qs[h] * grown, cot, 0, 0) - y[:, hd:]
        bc_ref[h] = jnp.concatenate([b, c], axis=1).astype(bf16)
        x_ref[h] = x[:, :hd].astype(bf16)
        z_ref[h] = x[:, hd:]
        u_ref[h] = inverse[h]


def kernel_compose(bc_ref, other_ref, *outs, full):
    heads, hd = bc_ref.shape[0], bc_ref.shape[1]
    first = jnp.full((hd, 2 * hd), place_core(), jnp.int32) == 0
    for h in range(heads):
        a = bc_ref[h].astype(f32)
        b = other_ref[h].astype(f32)
        early = jnp.where(first, a, b)
        late = jnp.where(first, b, a)
        joined = mm(early[:, :hd], late if full else late[:, hd:])
        c = joined[:, -hd:] + early[:, hd:]
        outs[0][h] = c.astype(bf16)
        if full:
            outs[1][h] = jnp.concatenate([joined[:, :hd], c], axis=1).astype(bf16)


def kernel_b(gates_ref, x_ref, z0_ref, other_ref, *refs, count, steps):
    received = refs[:count]
    outs = refs[count : count + steps]
    z_ref, end_ref, dv_ref = refs[count + steps :]
    heads, n, hd = x_ref.shape
    me = place_level()
    last = jnp.full((hd, hd), place_core(), jnp.int32) == 1
    strengths = to_columns([sigmoid(gates_ref[1, h : h + 1, :]) for h in range(heads)])
    for h in range(heads):
        end = jnp.zeros((hd, hd), f32)
        for index, ref in reversed(list(enumerate(received))):
            if index == count - 1:
                end = ref[h].astype(f32)
            else:
                end = mm(ref[h, :, :hd], end) + ref[h, :, hd:].astype(f32)
        inner = mm(other_ref[h, :, :hd], end) + other_ref[h, :, hd:].astype(f32)
        end = jnp.where(last, end, inner)
        z = z0_ref[h] + mm(x_ref[h], end)
        z_ref[h] = z
        end_ref[h] = end
        dv_ref[:, h * hd : (h + 1) * hd] = strengths[h] * z
    block = n // steps
    for m in range(steps):
        at = pl.multiple_of((me ^ m) * block, block)
        outs[m][...] = dv_ref[pl.ds(at, block), :].astype(bf16)


def kernel_early(
    gates_ref,
    params_ref,
    tokens_ref,
    s_ref,
    u_ref,
    ut_ref,
    fade_ref,
    sink_ref,
    gram_ref,
    cross_ref,
    ks_ref,
    qn_ref,
    kn_ref,
    dq_ref,
    side_ref,
):
    q_ref, k_ref, g_ref = thirds(tokens_ref)
    heads, n, hd = qn_ref.shape
    i, j = positions(n)
    rows, sums, sum_rows, strengths = shared(gates_ref, params_ref, heads, i, j)
    sides = []
    for h in range(heads):
        qraw, qinv = units(q_ref, h, hd)
        kraw, kinv = units(k_ref, h, hd)
        q = qraw * qinv * hd ** (-0.5)
        k = kraw * kinv
        last = sums[h][n - 1 : n, :]
        tail = jnp.exp(last - sums[h])
        grown = jnp.exp(sums[h])
        fade = jnp.where(i <= j, jnp.exp(jnp.where(i <= j, sum_rows[h] - sums[h], 0.0)), 0.0)
        state = s_ref[h]
        ut_ref[h] = u_ref[h].T.astype(bf16)
        fade_ref[h] = fade
        sink_ref[h] = jnp.where(i < j, -fade * rows[h][1], 0.0)
        gram_ref[h] = mm(k, k, 1, 1)
        cross_ref[h] = mm(k, q, 1, 1)
        ks_ref[h] = grown * mm(k, state)
        qn_ref[h] = q.astype(bf16)
        kn_ref[h] = k.astype(bf16)
        dq_in = grown * mm(g_ref[:, h * hd : (h + 1) * hd], state, 1, 1)
        dq_ref[h] = dq_in
        sides += [
            jnp.sum(q * dq_in, axis=1, keepdims=True),
            tail,
            strengths[h],
            grown,
            jnp.broadcast_to(jnp.exp(last), (n, 1)),
        ]
    side_ref[...] = jnp.concatenate(sides, axis=1)


def kernel_late(s_ref, kn_ref, side_ref, z_ref, end_ref, dk_ref, kend_ref, base_ref):
    heads, _, _ = z_ref.shape
    side = side_ref[...]
    bases = []
    for h in range(heads):
        inner, tail, strength, grown, all_decay = [
            side[:, 5 * h + index : 5 * h + index + 1] for index in range(5)
        ]
        state = s_ref[h]
        end = end_ref[h]
        k = kn_ref[h]
        dk_in = -grown * mm(strength * z_ref[h], state, 1, 1)
        dk_ref[h] = dk_in
        kend_ref[h] = tail * mm(k, end)
        bases.append(inner + jnp.sum(k.astype(f32) * dk_in, axis=1, keepdims=True))
        total = jnp.sum(jnp.sum(state * end, axis=1, keepdims=True), axis=0, keepdims=True)
        bases.append(all_decay * total)
    base_ref[...] = jnp.concatenate(bases, axis=1)


def kernel_gates(
    gates_ref,
    params_ref,
    tokens_ref,
    z_ref,
    ut_ref,
    fade_ref,
    sink_ref,
    gram_ref,
    cross_ref,
    ks_ref,
    kend_ref,
    side_ref,
    base_ref,
    *refs,
    steps,
):
    g_ref = thirds(tokens_ref)[2]
    v_in = refs[:steps]
    gate_ref, small_ref, both_ref, new_ref, v_ref = refs[steps:]
    heads, n, hd = z_ref.shape
    me = place_level()
    block = n // steps
    for m in range(steps):
        at = pl.multiple_of((me ^ m) * block, block)
        v_ref[pl.ds(at, block), :] = v_in[m][...].astype(f32)
    i, j = positions(n)
    rows = gate_rows(gates_ref, params_ref, heads)
    side = side_ref[...]
    bases = base_ref[...]
    changes, products, sums, extra = [], [], [], []
    for h in range(heads):
        cols = slice(h * hd, (h + 1) * hd)
        base = bases[:, 2 * h : 2 * h + 1]
        strength = side[:, 5 * h + 2 : 5 * h + 3]
        z = z_ref[h]
        new = mm(ut_ref[h], strength * (v_ref[:, cols] - ks_ref[h]))
        near = fade_ref[h] * mm(new, g_ref[:, cols], 1, 1)
        solve = sink_ref[h] * mm(new, z, 1, 1)
        both_ref[h, :, :n] = near.astype(bf16)
        both_ref[h, :, n:] = solve.astype(bf16)
        new_ref[h] = new.astype(bf16)
        pairs = near * cross_ref[h] + solve * gram_ref[h]
        weight = jnp.sum(new * kend_ref[h], axis=1, keepdims=True)
        changes.append(base - jnp.sum(pairs, axis=1, keepdims=True) - weight)
        products.append(jnp.sum(z * new, axis=1, keepdims=True))
        sums.append(jnp.sum(pairs, axis=0, keepdims=True))
        extra.append(jnp.sum(weight, axis=0, keepdims=True) + bases[0:1, 2 * h + 1 : 2 * h + 2])
    from_rows = to_columns(sums)
    strength_rows = to_rows(products)
    si = lax.broadcasted_iota(jnp.int32, small_ref.shape, 0)
    sj = lax.broadcasted_iota(jnp.int32, small_ref.shape, 1)
    small = jnp.zeros(small_ref.shape, f32)
    for h in range(heads):
        change = changes[h] + from_rows[h]
        dlog = jnp.sum(jnp.where(i >= j, change, 0.0), axis=0, keepdims=True) + extra[h]
        dgate = dlog * rows[h][2]
        gate_ref[0, h : h + 1, :] = dgate
        gate_ref[1, h : h + 1, :] = strength_rows[h] * (1.0 - rows[h][1])
        first = jnp.sum(dlog * rows[h][0], axis=1, keepdims=True)
        second = jnp.sum(dgate, axis=1, keepdims=True)
        small = small + jnp.where((si == 0) & (sj == h), first, 0.0)
        small = small + jnp.where((si == 1) & (sj == h), second, 0.0)
    small_ref[...] = small


def kernel_units(
    tokens_ref, qn_ref, kn_ref, end_ref, dq_in_ref, dk_in_ref, side_ref, both_ref, new_ref, *outs
):
    dq_ref, dk_ref = outs
    q_ref, k_ref, _ = thirds(tokens_ref)
    heads, n, hd = new_ref.shape
    side = side_ref[...]
    for h in range(heads):
        cols = slice(h * hd, (h + 1) * hd)
        qraw, qinv = units(q_ref, h, hd)
        kraw, kinv = units(k_ref, h, hd)
        tail = side[:, 5 * h + 1 : 5 * h + 2]
        both = both_ref[h]
        by_key = mm(both, kn_ref[h], 0, 0)
        dq = by_key[:n] + dq_in_ref[h]
        dk = (
            mm(both[:, :n], qn_ref[h])
            + mm(both[:, n:], kn_ref[h])
            + by_key[n:]
            + dk_in_ref[h]
            + tail * mm(new_ref[h], end_ref[h], 1, 1)
        )
        dq = (hd ** (-0.5)) * (
            qinv * dq - qraw * (qinv * qinv * qinv * jnp.sum(qraw * dq, axis=1, keepdims=True))
        )
        dk = kinv * dk - kraw * (kinv * kinv * kinv * jnp.sum(kraw * dk, axis=1, keepdims=True))
        dq_ref[:, cols] = dq.astype(bf16)
        dk_ref[:, cols] = dk.astype(bf16)


def pieces(group):
    return sum(2 if m % 4 == 3 else 1 for m in group)


def pick(level, m, refs, scratch):
    if m % 4 != 3:
        return refs.pop(0)[...]
    straight, relayed = refs.pop(0), refs.pop(0)
    outer = (level + 1) % 4 < 2

    @pl.when(outer)
    def _():
        scratch[...] = relayed[...]

    @pl.when(jnp.logical_not(outer))
    def _():
        scratch[...] = straight[...]

    return scratch[...]


def kernel_values(*refs, chips, group):
    tokens = refs[:chips]
    chunks = pieces(group)
    mine = list(refs[chips : chips + chunks])
    theirs = list(refs[chips + chunks : chips + 2 * chunks])
    outs = refs[chips + 2 * chunks : -1]
    scratch = refs[-1]
    core = place_core()
    level = place_level()
    block = tokens[0].shape[0]
    part, width = mine[0].shape
    own_at = pl.multiple_of(core * part, part)
    other_at = pl.multiple_of((1 - core) * part, part)
    own = jnp.concatenate([ref[:, pl.ds(own_at, part)] for ref in tokens], axis=0)
    other = jnp.concatenate([ref[:, pl.ds(other_at, part)] for ref in tokens], axis=0)
    for m, number in enumerate(group):
        result = jnp.dot(
            own, pick(level, number, mine, scratch.at[0]), preferred_element_type=f32
        ) + jnp.dot(other, pick(level, number, theirs, scratch.at[1]), preferred_element_type=f32)
        for s in range(chips):
            outs[s][:, m * width : (m + 1) * width] = result[s * block : (s + 1) * block].astype(
                bf16
            )


def kernel_cut(tokens_hbm, *refs):
    outs, sems = refs[:-1], refs[-1]
    width = outs[0].shape[1]
    copies = []
    for s, out in enumerate(outs):
        at = pl.multiple_of((place_chip() ^ s) * width, width)
        copies.append(pltpu.make_async_copy(tokens_hbm.at[:, pl.ds(at, width)], out, sems.at[s]))
    for copy in copies:
        copy.start()
    for copy in copies:
        copy.wait()


def kernel_sum(*refs, chips):
    total = refs[0][...].astype(f32)
    for ref in refs[1:chips]:
        total = total + ref[...].astype(f32)
    outs = refs[chips:]
    width = outs[0].shape[1]
    for m, out_ref in enumerate(outs):
        out_ref[...] = total[:, m * width : (m + 1) * width].astype(out_ref.dtype)


def kernel_input(*refs, chips, group, first, final):
    grads, refs = refs[:2], refs[2:]
    chunks = pieces(group)
    mine = list(refs[:chunks])
    theirs = list(refs[chunks : 2 * chunks])
    rest = list(refs[2 * chunks :])
    before = None if first else rest.pop(0)
    scratch = rest.pop()
    core = place_core()
    level = place_level()
    block = 2 * grads[0].shape[0] // chips
    part, width = mine[0].shape
    rows = jnp.concatenate([ref[...] for ref in grads], axis=0)
    for index, (found, at) in enumerate(((mine, core * part), (theirs, (1 - core) * part))):
        total = None if first else before[index]
        for m in group:
            piece = lax.dot_general(
                rows[:, m * width : (m + 1) * width],
                pick(level, m, found, scratch.at[index]),
                (((1,), (1,)), ((), ())),
                preferred_element_type=f32,
            )
            total = piece if total is None else total + piece
        if final:
            place = pl.multiple_of(at, part)
            for s in range(chips):
                rest[s][:, pl.ds(place, part)] = total[s * block : (s + 1) * block].astype(bf16)
        else:
            rest[0][index] = total


def kernel_assemble(*refs, chips):
    small, parts = refs[:chips], refs[chips : 2 * chips]
    out_ref, decay_ref = refs[2 * chips :]
    width = parts[0].shape[1]
    me = place_chip()
    for s, ref in enumerate(parts):
        at = pl.multiple_of((me ^ s) * width, width)
        out_ref[:, pl.ds(at, width)] = ref[...]
    total = functools.reduce(jnp.add, [ref[...] for ref in small])
    decay_ref[...] = total[: decay_ref.shape[0], : decay_ref.shape[1]]


def kernel_stack(first_ref, second_ref, out_ref):
    n = first_ref.shape[0]
    out_ref[:n, :] = first_ref[...]
    out_ref[n:, :] = second_ref[...]


def kernel_join(*refs):
    out_ref = refs[-1]
    width = refs[0].shape[1]
    for m, ref in enumerate(refs[:-1]):
        out_ref[:, m * width : (m + 1) * width] = ref[...]


def kernel_decay(*refs):
    out_ref = refs[-1]
    total = functools.reduce(jnp.add, [ref[...] for ref in refs[:-1]])
    out_ref[...] = total[: out_ref.shape[0], : out_ref.shape[1]]


def struct(shape, kind):
    return jax.ShapeDtypeStruct(shape, kind)


VMEM = pl.BlockSpec(memory_space=pltpu.VMEM)
HBM = pl.BlockSpec(memory_space=pltpu.HBM)


def call(body, args, specs, outs, scratch=()):
    return pl.pallas_call(
        body,
        in_specs=list(specs),
        out_specs=[VMEM] * len(outs),
        out_shape=list(outs),
        scratch_shapes=list(scratch),
        cost_estimate=pl.CostEstimate(
            flops=3 * 10**9, bytes_accessed=20 * 10**6, transcendentals=0
        ),
        compiler_params=pltpu.CompilerParams(vmem_limit_bytes=12 * 1024 * 1024),
    )(*args)


def weight_order(steps):
    return sorted(range(1, steps), key=lambda m: (m // 4, (-m) % 2, m))


def per_device(
    layer_input, value_weight, query_raw, key_raw, out_grad, gate_logits, decay_params, saved_states
):
    plane = ("dp", "ctx")
    cores = 2
    blocks = lax.axis_size("ctx")
    members = lax.axis_size("dp") * blocks
    chips = members // cores
    steps = lax.axis_size("tp")
    tokens = layer_input[0]
    block, model = tokens.shape
    part, width = value_weight.shape
    hd = saved_states.shape[-1]
    heads = query_raw.shape[2] // hd
    length = query_raw.shape[1]
    q, k, g = query_raw[0], key_raw[0], out_grad[0]
    gates = gate_logits[:, 0]
    stacked = jnp.concatenate([q, k, g])
    states = saved_states[0, 0]

    def turn(array, m, places=None):
        pairs = [(t, t ^ m) for t in range(steps) if places is None or t in places]
        return lax.ppermute(array, "tp", pairs)

    def swap(array):
        return lax.ppermute(array, plane, [(p, p ^ 1) for p in range(members)])

    def cross(array, s):
        return lax.ppermute(array, plane, [(p, p ^ (cores * s)) for p in range(members)])

    mine = {0: (value_weight,)}
    for m in weight_order(steps):
        if m % 4 == 3:
            inner = [t for t in range(steps) if t % 4 in (1, 2)]
            straight = turn(value_weight, m, inner)
            relayed = turn(mine[m - 1][0], 1, inner)
            mine[m] = (straight, relayed)
        else:
            mine[m] = (turn(value_weight, m),)
    theirs = {m: tuple(swap(a) for a in mine[m]) for m in range(steps)}

    def chunks(found, group):
        return [a for m in group for a in found[m]]

    bc, x1, z0, inverse = call(
        kernel_a,
        (gates, decay_params, stacked),
        (VMEM, VMEM, VMEM),
        (
            struct((heads, hd, 2 * hd), bf16),
            struct((heads, length, hd), bf16),
            struct((heads, length, hd), f32),
            struct((heads, length, length), f32),
        ),
    )
    other = swap(bc)
    ranks = blocks // cores
    full = ranks > 2
    joined = call(
        functools.partial(kernel_compose, full=full),
        (bc, other),
        (VMEM, VMEM),
        (struct((heads, hd, hd), bf16),) + ((struct((heads, hd, 2 * hd), bf16),) if full else ()),
    )
    received = []
    for d in range(1, ranks):
        received.append(
            lax.ppermute(
                joined[1] if d < ranks - 1 else joined[0],
                "ctx",
                [(p, p - cores * d) for p in range(cores * d, blocks)],
            )
        )

    cuts = call(
        kernel_cut,
        (tokens,),
        (HBM,),
        tuple(struct((block, cores * part), bf16) for _ in range(chips)),
        scratch=(pltpu.SemaphoreType.DMA((chips,)),),
    )
    token_parts = [cuts[s] if s == 0 else cross(cuts[s], s) for s in range(chips)]

    outs = call(
        functools.partial(kernel_b, count=len(received), steps=steps),
        (gates, x1, z0, other, *received),
        (VMEM,) * (4 + len(received)),
        tuple(struct((block, width), bf16) for _ in range(steps))
        + (struct((heads, length, hd), f32), struct((heads, hd, hd), f32)),
        scratch=(pltpu.VMEM((length, width), f32),),
    )
    dv_blocks, z, end = outs[:steps], outs[steps], outs[steps + 1]
    dv_cols = [dv_blocks[m] if m == 0 else turn(dv_blocks[m], m) for m in range(steps)]
    dv_row = call(
        kernel_join, tuple(dv_cols), (VMEM,) * steps, (struct((block, steps * width), bf16),)
    )[0]
    dv_parts = [dv_row]
    for e in range((chips - 1).bit_length()):
        if e:
            dv_row = call(
                kernel_stack,
                tuple(dv_parts),
                (VMEM,) * 2,
                (struct((2 * dv_row.shape[0], dv_row.shape[1]), bf16),),
            )[0]
        dv_parts = [dv_row, cross(dv_row, 2**e)]


    groups = [tuple(range(steps - 1)), (steps - 1,)]
    v_blocks = []
    for group in groups:
        sums = call(
            functools.partial(kernel_values, chips=chips, group=group),
            (*token_parts, *chunks(mine, group), *chunks(theirs, group)),
            (VMEM,) * (chips + 2 * len(chunks(mine, group))),
            tuple(struct((block, width * len(group)), bf16) for _ in range(chips)),
            scratch=(pltpu.VMEM((2, part, width), bf16),),
        )
        back = [sums[s] if s == 0 else cross(sums[s], s) for s in range(chips)]
        whole = call(
            functools.partial(kernel_sum, chips=chips),
            tuple(back),
            (VMEM,) * chips,
            tuple(struct((block, width), bf16) for _ in group),
        )
        v_blocks += [part_v if m == 0 else turn(part_v, m) for m, part_v in zip(group, whole)]

    acc = None
    for group in groups:
        first, final = group is groups[0], group is groups[-1]
        args = (*dv_parts, *chunks(mine, group), *chunks(theirs, group)) + (
            () if first else (acc,)
        )
        res = call(
            functools.partial(kernel_input, chips=chips, group=group, first=first, final=final),
            args,
            (VMEM,) * len(args),
            tuple(struct((block, cores * part), bf16) for _ in range(chips))
            if final
            else (struct((cores, chips * block, part), f32),),
            scratch=(pltpu.VMEM((2, part, width), bf16),),
        )
        if final:
            in_blocks = res
        else:
            acc = res[0]
    in_back = [in_blocks[s] if s == 0 else cross(in_blocks[s], s) for s in range(chips)]
    square = struct((heads, length, length), f32)
    tall = struct((heads, length, hd), f32)
    tall_half = struct((heads, length, hd), bf16)
    ut, fade, sink, gram, cross_prod, k_state, qn, kn, dq_in, side = call(
        kernel_early,
        (gates, decay_params, stacked, states, inverse),
        (VMEM,) * 5,
        (
            struct((heads, length, length), bf16),
            square,
            square,
            square,
            square,
            tall,
            tall_half,
            tall_half,
            tall,
            struct((length, 5 * heads), f32),
        ),
    )
    dk_in, k_end, base = call(
        kernel_late,
        (states, kn, side, z, end),
        (VMEM,) * 5,
        (tall, tall, struct((length, 2 * heads), f32)),
    )
    gate, small, both, new = call(
        functools.partial(kernel_gates, steps=steps),
        (
            gates,
            decay_params,
            stacked,
            z,
            ut,
            fade,
            sink,
            gram,
            cross_prod,
            k_state,
            k_end,
            side,
            base,
            *v_blocks,
        ),
        (VMEM,) * (13 + steps),
        (
            struct((2, heads, length), f32),
            struct((8, 128), f32),
            struct((heads, length, 2 * length), bf16),
            tall_half,
        ),
        scratch=(pltpu.VMEM((length, width), f32),),
    )
    dq, dk = call(
        kernel_units,
        (stacked, qn, kn, end, dq_in, dk_in, side, both, new),
        (VMEM,) * 9,
        (struct((length, width), bf16), struct((length, width), bf16)),
    )
    tile = (struct(small.shape, f32),)
    small = call(kernel_decay, (small, swap(small)), (VMEM, VMEM), tile)[0]
    shares = [small if s == 0 else cross(small, s) for s in range(chips)]
    input_grad, decay_grad = call(
        functools.partial(kernel_assemble, chips=chips),
        (*shares, *in_back),
        (VMEM,) * (2 * chips),
        (struct((block, model), bf16), struct((2, heads), f32)),
    )
    return (input_grad[None], dq[None], dk[None], gate[:, None], decay_grad)


def solution(mesh):
    placed = (
        P("dp", ("ctx", "tp"), None),
        P(("dp", "ctx"), "tp"),
        P("dp", "ctx", "tp"),
        P("dp", "ctx", "tp"),
        P("dp", "ctx", "tp"),
        P(None, "dp", "tp", "ctx"),
        P(None, "tp"),
        P("dp", "ctx", "tp", None, None),
    )
    return jax.shard_map(
        per_device,
        mesh=mesh,
        in_specs=placed,
        out_specs=(
            P("dp", ("ctx", "tp"), None),
            P("dp", "ctx", "tp"),
            P("dp", "ctx", "tp"),
            P(None, "dp", "tp", "ctx"),
            P(None, "tp"),
        ),
        check_vma=False,
    )
```
